32 devices in a mesh: seq: 8 (over y, x, core), head: 4 (over z).
Axes of the slice: x: 2, y: 2, z: 4, core: 2. Of those that a mesh axis runs over, the one named last changes fastest.
Arguments:
- queries: bfloat16 [4096, 4096], P('seq', 'head'), may hold values from -7 to 7
- keys: bfloat16 [32768, 1024], P('seq', 'head'), may hold values from -4 to 4
- values: bfloat16 [32768, 1024], P('seq', 'head'), may hold values from -5 to 5
- out_grad: bfloat16 [4096, 4096], P('seq', 'head'), may hold values from -6 to 6
- out_weight: bfloat16 [4096, 4096], P('head'), may hold values from -0.09375 to 0.09375
- selected: int32 [8, 6], replicated, may hold values from 0 to 63, as said below
Outputs:
- query_grad: bfloat16 [4096, 4096], P('seq', 'head')
- key_grad: bfloat16 [32768, 1024], P('seq', 'head')
- value_grad: bfloat16 [32768, 1024], P('seq', 'head')
The draws below stay inside these ranges and needn't reach their ends.
Inputs may be any that keep to these rules, and one draw needn't show every extreme that they name: `selected`: row i lists first the block i * 8 + 7, then 5 further distinct blocks of lower number; among them at most one lies in the run of 8 blocks j * 8 to j * 8 + 7 of any j other than i, and every row i >= 1 lists exactly one block of the run of j = 0.
All inputs are finite; a program needn't handle non-finite values.
Results may differ from the reference program's by a relative error of at most 0.0095.
Values may be sent and summed in bfloat16 or wider, within the bound.
No kernel may reach another device: no remote copies, remote signals or barrier semaphores. Data moves between devices by JAX's collectives and lax.ppermute only.
A program may use at most 128 MiB of HBM per device.

```python
import jax
import jax.numpy as jnp
from jax import lax

D = 4096
HEADS = 32
KV_HEADS = 8
HEAD_DIM = 128
BLOCK = 512
TOPK = 6
KB_DEV = 8
QBLOCKS = 8
QUERIES = 4096
KBLOCKS = 64
KEYS = 32768


def draw_queries(key, part):
    noise = jax.random.normal(jax.random.fold_in(key, 11), (QUERIES, HEADS * HEAD_DIM), jnp.float32)
    base = jnp.clip(noise, -4.0, 4.0)
    return base.astype(jnp.bfloat16)


def draw_keys(key, part):
    noise = jax.random.normal(jax.random.fold_in(key, 13), (KEYS, KV_HEADS * HEAD_DIM), jnp.float32)
    base = jnp.clip(noise, -4.0, 4.0)
    return base.astype(jnp.bfloat16)


def draw_selected(key, part):
    row_count = QBLOCKS
    row_index = jnp.arange(row_count, dtype=jnp.int32)[:, None]
    owner_index = jnp.arange(row_count, dtype=jnp.int32)[None, :]
    offsets = jax.random.randint(jax.random.fold_in(key, 21), (row_count, row_count), 0, KB_DEV, dtype=jnp.int32)
    remote_blocks = owner_index * KB_DEV + offsets
    local_blocks = jnp.broadcast_to(row_index * KB_DEV + jnp.arange(KB_DEV - 1, dtype=jnp.int32)[None, :], (row_count, KB_DEV - 1))
    remote_draw = jax.random.randint(jax.random.fold_in(key, 22), (row_count, row_count), 0, 1024, dtype=jnp.int32)
    remote_draw = jnp.where(owner_index == 0, 2048, remote_draw)
    remote_score = jnp.where(owner_index < row_index, remote_draw, -1)
    local_score = jax.random.randint(jax.random.fold_in(key, 23), (row_count, KB_DEV - 1), 0, 256, dtype=jnp.int32)
    scores = jnp.concatenate([local_score, remote_score], axis=1)
    width_all = scores.shape[1]
    ranked = scores * width_all + jnp.arange(width_all, dtype=jnp.int32)[None, :]
    unused_values, chosen = lax.top_k(ranked, TOPK - 1)
    candidates = jnp.concatenate([local_blocks, remote_blocks], axis=1)
    picked = jnp.take_along_axis(candidates, chosen, axis=1)
    own_block = row_index * KB_DEV + KB_DEV - 1
    return jnp.concatenate([own_block, picked], axis=1).astype(jnp.int32)


def block_scale(own_key, dims, cuts, least, largest):
    level, own = 1.0, jax.random.fold_in(own_key, 6)
    for dim, shards_of in cuts:
        heights = jnp.exp(jax.random.uniform(jax.random.fold_in(own, dim), (shards_of,), jnp.float32, least / len(cuts), largest / len(cuts)))
        level = level * jnp.repeat(heights, dims[dim] // shards_of).reshape([-1 if axis == dim else 1 for axis in range(len(dims))])
    return level


def scatter_about(stream_key, dims, width, most, pieces=(), kind=jnp.bfloat16):
    result = width * jax.random.normal(stream_key, dims, jnp.float32)
    if pieces:
        result = result * block_scale(stream_key, dims, pieces, -0.22, 0.18)
    return jnp.clip(result, -most, most).astype(kind)


def setup_inputs(seed: int = 0) -> dict:
    streams_of = jax.random.split(jax.random.key(seed), 7)
    queries = draw_queries(jax.random.fold_in(streams_of[6], 71), 0)
    keys = draw_keys(jax.random.fold_in(streams_of[6], 71), 0)
    values = scatter_about(streams_of[2], (KEYS, KV_HEADS * HEAD_DIM), 1.0, 5.0, ((0, 8), (1, 4)))
    out_grad = scatter_about(streams_of[3], (QUERIES, D), 1.0, 6.0, ((0, 8), (1, 4)))
    out_weight = scatter_about(streams_of[4], (HEADS * HEAD_DIM, D), (HEADS * HEAD_DIM) ** -0.5, 0.09375, ((0, 4),))
    selected = draw_selected(jax.random.fold_in(streams_of[6], 71), 0)
    return {"queries": queries, "keys": keys, "values": values, "out_grad": out_grad, "out_weight": out_weight, "selected": selected}


def head_block(query_tile, grad_tile, key_tile, value_tile, visible):
    factor = HEAD_DIM ** -0.5
    query_f = query_tile.astype(jnp.float32)
    grad_f = grad_tile.astype(jnp.float32)
    key_f = key_tile.astype(jnp.float32)
    value_f = value_tile.astype(jnp.float32)
    scores = jnp.einsum("gqd,kd->gqk", query_f, key_f) * factor
    scores = jnp.where(visible, scores, -jnp.inf)
    row_max = jnp.max(scores, axis=-1, keepdims=True)
    shifted = jnp.exp(scores - row_max)
    weights = shifted / jnp.sum(shifted, axis=-1, keepdims=True)
    weights_low = lax.optimization_barrier(weights.astype(jnp.bfloat16)).astype(jnp.float32)
    attended = jnp.einsum("gqk,kd->gqd", weights_low, value_f)
    row_dot = jnp.sum(grad_f * attended, axis=-1, keepdims=True)
    value_part = jnp.einsum("gqk,gqd->kd", weights_low, grad_f)
    grad_weights = jnp.einsum("gqd,kd->gqk", grad_f, value_f)
    grad_scores = weights * (grad_weights - row_dot)
    grad_low = lax.optimization_barrier(grad_scores.astype(jnp.bfloat16)).astype(jnp.float32)
    query_part = jnp.einsum("gqk,kd->gqd", grad_low, key_f) * factor
    key_part = jnp.einsum("gqk,gqd->kd", grad_low, query_f) * factor
    return query_part, key_part, value_part


def reference(queries, keys, values, out_grad, out_weight, selected):
    group_size = HEADS // KV_HEADS
    grad_output = jnp.dot(out_grad, out_weight.T, preferred_element_type=jnp.float32).astype(jnp.bfloat16)
    key_tiles = keys.reshape(KBLOCKS, BLOCK, KV_HEADS, HEAD_DIM)
    value_tiles = values.reshape(KBLOCKS, BLOCK, KV_HEADS, HEAD_DIM)
    query_tiles = queries.reshape(QBLOCKS, BLOCK, KV_HEADS, group_size, HEAD_DIM)
    grad_tiles = grad_output.reshape(QBLOCKS, BLOCK, KV_HEADS, group_size, HEAD_DIM)
    length = TOPK * BLOCK
    column = jnp.arange(length, dtype=jnp.int32)[None, :]
    rowpos = jnp.arange(BLOCK, dtype=jnp.int32)[:, None]
    visible = (column >= BLOCK) | (column <= rowpos)

    def per_head(operands):
        query_tile, grad_tile, key_tile, value_tile = operands
        return head_block(query_tile, grad_tile, key_tile, value_tile, visible)

    def one_block(totals, number):
        key_sum, value_sum = totals
        chosen = lax.dynamic_index_in_dim(selected, number, 0, keepdims=False).astype(jnp.int32)
        key_pick = jnp.take(key_tiles, chosen, axis=0).reshape(length, KV_HEADS, HEAD_DIM)
        value_pick = jnp.take(value_tiles, chosen, axis=0).reshape(length, KV_HEADS, HEAD_DIM)
        query_block = lax.dynamic_index_in_dim(query_tiles, number, 0, keepdims=False)
        grad_block = lax.dynamic_index_in_dim(grad_tiles, number, 0, keepdims=False)
        query_part, key_part, value_part = lax.map(per_head, (query_block.transpose(1, 2, 0, 3), grad_block.transpose(1, 2, 0, 3), key_pick.transpose(1, 0, 2), value_pick.transpose(1, 0, 2)))
        query_out = query_part.transpose(2, 0, 1, 3).reshape(BLOCK, HEADS * HEAD_DIM).astype(jnp.bfloat16)
        key_low = lax.optimization_barrier(key_part.astype(jnp.bfloat16)).astype(jnp.float32)
        value_low = lax.optimization_barrier(value_part.astype(jnp.bfloat16)).astype(jnp.float32)
        key_add = key_low.transpose(1, 0, 2).reshape(TOPK, BLOCK, KV_HEADS, HEAD_DIM)
        value_add = value_low.transpose(1, 0, 2).reshape(TOPK, BLOCK, KV_HEADS, HEAD_DIM)
        key_sum = key_sum.at[chosen].add(key_add)
        value_sum = value_sum.at[chosen].add(value_add)
        return (key_sum, value_sum), query_out

    initial = (jnp.zeros((KBLOCKS, BLOCK, KV_HEADS, HEAD_DIM), jnp.float32), jnp.zeros((KBLOCKS, BLOCK, KV_HEADS, HEAD_DIM), jnp.float32))
    (key_sum, value_sum), query_rows = lax.scan(one_block, initial, jnp.arange(QBLOCKS, dtype=jnp.int32))
    query_grad = query_rows.reshape(QUERIES, HEADS * HEAD_DIM)
    key_grad = key_sum.reshape(KEYS, KV_HEADS * HEAD_DIM).astype(jnp.bfloat16)
    value_grad = value_sum.reshape(KEYS, KV_HEADS * HEAD_DIM).astype(jnp.bfloat16)
    return (query_grad, key_grad, value_grad)
```

```python
import functools
import math

import jax
import jax.numpy as jnp
from jax import lax
from jax.experimental import pallas as pl
from jax.experimental.pallas import tpu as pltpu
from jax.sharding import PartitionSpec as P


HEAD_DIM = 128
BLOCK = 512
TOPK = 6
CHUNKS = 2
HIDDEN = -1e30


HBM = pl.BlockSpec(memory_space=pltpu.HBM)
ANY = pl.BlockSpec(memory_space=pltpu.HBM)
SMEM = pl.BlockSpec(memory_space=pltpu.SMEM)
VMEM_LIMIT = 60 * 1024 * 1024
PARTS = 2
SPAN = 3
NT = (((1,), (1,)), ((), ()))


def pick_of(sel_ref, row, owner, blocks_here):
    found = jnp.int32(-1)
    for slot in range(TOPK):
        block = sel_ref[row, slot]
        found = jnp.where(block // blocks_here == owner, block % blocks_here, found)
    return found


def pack_kernel(head, devices, blocks_here, sel_ref, pos_ref, keys_ref, values_ref, out_ref, buf, in_sem, out_sem):
    here = pos_ref[0]
    cols = pl.ds(head * HEAD_DIM, HEAD_DIM)

    def loads(shift, inner):
        rows = pl.ds(pl.multiple_of(inner * BLOCK, BLOCK), BLOCK)
        slot = buf.at[shift]
        return (
            pltpu.make_async_copy(keys_ref.at[rows, cols], slot.at[pl.ds(0, BLOCK)], in_sem.at[shift, 0]),
            pltpu.make_async_copy(values_ref.at[rows, cols], slot.at[pl.ds(BLOCK, BLOCK)], in_sem.at[shift, 1]),
        )

    def store(shift):
        return pltpu.make_async_copy(buf.at[shift], out_ref.at[here + shift], out_sem.at[shift])

    for shift in range(1, devices):
        @pl.when(here + shift < devices)
        def _():
            inner = jnp.maximum(pick_of(sel_ref, here + shift, here, blocks_here), 0)
            for copy in loads(shift, inner):
                copy.start()

    for shift in range(1, devices):
        @pl.when(here + shift < devices)
        def _():
            for copy in loads(shift, 0):
                copy.wait()
            store(shift).start()

    for shift in range(1, devices):
        @pl.when(here + shift < devices)
        def _():
            store(shift).wait()


def pack(head, devices, blocks_here, selected, position, keys, values):
    shape = (devices, 2 * BLOCK, HEAD_DIM)
    return pl.pallas_call(
        functools.partial(pack_kernel, head, devices, blocks_here),
        out_shape=jax.ShapeDtypeStruct(shape, jnp.bfloat16),
        in_specs=[SMEM, SMEM, HBM, HBM],
        out_specs=HBM,
        scratch_shapes=[
            pltpu.VMEM(shape, jnp.bfloat16),
            pltpu.SemaphoreType.DMA((devices, 2)),
            pltpu.SemaphoreType.DMA((devices,)),
        ],
        compiler_params=pltpu.CompilerParams(vmem_limit_bytes=VMEM_LIMIT),
    )(selected, position, keys, values)


def project_kernel(terms, chunks, place_ref, *refs):
    count = len(terms)
    og_refs, weight_ref, acc, og_buf, w_buf, sem = refs[: count * chunks], *refs[count * chunks :]
    here, groups = place_ref[0], place_ref[1]
    rows, depth = og_buf.shape[1] // chunks, og_buf.shape[2]

    def present(term):
        source = here + terms[term]
        return source, (source >= 0) & (source < groups)

    def copies(term, source):
        cols = pl.ds(pl.multiple_of(source * depth, depth), depth)
        made = [pltpu.make_async_copy(weight_ref.at[:, cols], w_buf.at[term], sem.at[term, 0])]
        for chunk in range(chunks):
            made.append(
                pltpu.make_async_copy(
                    og_refs[term * chunks + chunk],
                    og_buf.at[term, pl.ds(chunk * rows, rows)],
                    sem.at[term, 1 + chunk],
                )
            )
        return made

    for term in range(count):
        source, there = present(term)

        @pl.when(there)
        def _():
            for copy in copies(term, source):
                copy.start()

    for term in range(count):
        source, there = present(term)

        @pl.when(there)
        def _():
            for copy in copies(term, 0):
                copy.wait()
            product = lax.dot_general(
                og_buf[term], w_buf[term], NT, preferred_element_type=jnp.float32
            )
            acc[...] = product if terms[term] == 0 else acc[...] + product


def project(terms, arrays, weight, place):
    chunks = len(arrays[0])
    rows, depth = arrays[0][0].shape
    out_cols = weight.shape[0]
    flat = [part for term in arrays for part in term]
    return pl.pallas_call(
        functools.partial(project_kernel, terms, chunks),
        out_shape=jax.ShapeDtypeStruct((rows * chunks, out_cols), jnp.float32),
        in_specs=[SMEM] + [ANY] * len(flat) + [HBM],
        out_specs=pl.BlockSpec(memory_space=pltpu.VMEM),
        scratch_shapes=[
            pltpu.VMEM((len(terms), rows * chunks, depth), jnp.bfloat16),
            pltpu.VMEM((len(terms), out_cols, depth), jnp.bfloat16),
            pltpu.SemaphoreType.DMA((len(terms), 1 + chunks)),
        ],
        compiler_params=pltpu.CompilerParams(vmem_limit_bytes=VMEM_LIMIT),
        name="project",
    )(place, *flat, weight)


def weigh_kernel(head, blocks_here, has_old, *refs):
    sel_ref, pos_ref, q_ref, keys_ref, values_ref, recv_ref = refs[:6]
    refs = refs[11:] if has_old else refs[6:]
    p_ref, o_ref, i_ref, k_out, v_out, k_buf, v_buf, in_sem, out_sem = refs
    here = pos_ref[0]
    step = pl.program_id(0)
    rows = q_ref.shape[0]
    to_log2 = HEAD_DIM ** (-0.5) * math.log2(math.e)
    cols = pl.ds(head * HEAD_DIM, HEAD_DIM)

    def fetch(slot, key_src, value_src):
        where = pl.ds(slot * BLOCK, BLOCK)
        return (
            pltpu.make_async_copy(key_src, k_buf.at[where], in_sem.at[slot, 0]),
            pltpu.make_async_copy(value_src, v_buf.at[where], in_sem.at[slot, 1]),
        )

    def keep():
        return (
            pltpu.make_async_copy(k_buf, k_out.at[head], out_sem.at[0]),
            pltpu.make_async_copy(v_buf, v_out.at[head], out_sem.at[1]),
        )

    @pl.when(step == 0)
    def _():
        for slot in range(TOPK):
            block = sel_ref[here, slot]
            dist = here - block // blocks_here

            @pl.when(dist == 0)
            def _():
                src = pl.ds(pl.multiple_of(block % blocks_here * BLOCK, BLOCK), BLOCK)
                for copy in fetch(slot, keys_ref.at[src, cols], values_ref.at[src, cols]):
                    copy.start()

            if slot > 0:
                @pl.when(dist != 0)
                def _():
                    arrived = recv_ref.at[here - dist]
                    for copy in fetch(slot, arrived.at[pl.ds(0, BLOCK)], arrived.at[pl.ds(BLOCK, BLOCK)]):
                        copy.start()

        for slot in range(TOPK):
            first = pl.ds(0, BLOCK)
            for copy in fetch(slot, keys_ref.at[first, cols], values_ref.at[first, cols]):
                copy.wait()
        for copy in keep():
            copy.start()

    tile = rows // PARTS
    for part in range(PARTS):
        at = pl.ds(part * tile, tile)
        row = lax.broadcasted_iota(jnp.int32, (tile, BLOCK), 0) + part * tile
        visible = lax.broadcasted_iota(jnp.int32, (tile, BLOCK), 1) <= row
        scores = lax.dot_general(q_ref[at, :], k_buf[...], NT, preferred_element_type=jnp.float32)
        first = jnp.where(visible, scores[:, :BLOCK], HIDDEN)
        top = jnp.maximum(
            jnp.max(first, axis=1, keepdims=True), jnp.max(scores[:, BLOCK:], axis=1, keepdims=True)
        )
        total = jnp.zeros((tile, HEAD_DIM), jnp.float32)
        for slot in range(TOPK):
            piece = first if slot == 0 else scores[:, slot * BLOCK : (slot + 1) * BLOCK]
            raised = jnp.exp2((piece - top) * to_log2)
            for lane in range(BLOCK // HEAD_DIM):
                total = total + raised[:, lane * HEAD_DIM : (lane + 1) * HEAD_DIM]
            p_ref[0, slot, 0, at, :] = raised.astype(jnp.bfloat16)
        inverse = 1.0 / jnp.sum(total, axis=1, keepdims=True)
        attended = jnp.zeros((tile, HEAD_DIM), jnp.float32)
        for slot in range(TOPK):
            attended = attended + jnp.dot(
                p_ref[0, slot, 0, at, :], v_buf[pl.ds(slot * BLOCK, BLOCK), :], preferred_element_type=jnp.float32
            )
        o_ref[at, :] = attended * inverse
        i_ref[at, :] = jnp.broadcast_to(inverse, (tile, HEAD_DIM))

    @pl.when(step == pl.num_programs(0) - 1)
    def _():
        for copy in keep():
            copy.wait()


def weigh(head, kv_local, blocks_here, selected, position, queries, keys, values, recv, old):
    rows, q_cols = queries.shape
    group = q_cols // kv_local // HEAD_DIM
    length = TOPK * BLOCK
    slots = jax.ShapeDtypeStruct((kv_local, length, HEAD_DIM), jnp.bfloat16)
    wide = jax.ShapeDtypeStruct((rows, q_cols), jnp.float32)
    head_block = pl.BlockSpec((rows, HEAD_DIM), lambda g: (0, head * group + g))
    operands = [selected, position, queries, keys, values, recv]
    in_specs = [SMEM, SMEM, head_block, HBM, HBM, ANY]
    aliases = {}
    if old is not None:
        aliases = {len(operands) + n: n for n in range(5)}
        operands += list(old)
        in_specs += [HBM] * 5
    return pl.pallas_call(
        functools.partial(weigh_kernel, head, blocks_here, old is not None),
        grid=(group,),
        out_shape=[
            jax.ShapeDtypeStruct((kv_local, TOPK, group, rows, BLOCK), jnp.bfloat16), wide, wide, slots, slots,
        ],
        in_specs=in_specs,
        out_specs=[
            pl.BlockSpec((1, TOPK, 1, rows, BLOCK), lambda g: (head, 0, g, 0, 0)),
            head_block, head_block, HBM, HBM,
        ],
        scratch_shapes=[
            pltpu.VMEM((length, HEAD_DIM), jnp.bfloat16),
            pltpu.VMEM((length, HEAD_DIM), jnp.bfloat16),
            pltpu.SemaphoreType.DMA((TOPK, 2)),
            pltpu.SemaphoreType.DMA((2,)),
        ],
        input_output_aliases=aliases,
        compiler_params=pltpu.CompilerParams(vmem_limit_bytes=VMEM_LIMIT),
    )(*operands)


def send_piece(step, here, sel_ref, blocks_here, piece, back_ref, local_ref, sem):
    head, slot = step // TOPK, step % TOPK
    rows = pl.ds(pl.multiple_of(head * BLOCK, BLOCK), BLOCK)
    dist = here - sel_ref[here, slot] // blocks_here

    @pl.when(dist == 0)
    def _():
        pltpu.make_async_copy(piece.at[step], local_ref.at[slot, rows], sem.at[step]).start()

    @pl.when(dist != 0)
    def _():
        pltpu.make_async_copy(piece.at[step], back_ref.at[here - dist, rows], sem.at[step]).start()

    @pl.when(step == piece.shape[0] - 1)
    def _():
        for index in range(piece.shape[0]):
            pltpu.make_async_copy(piece.at[index], local_ref.at[0, pl.ds(0, BLOCK)], sem.at[index]).wait()


def values_kernel(blocks_here, group, chunks, late, *refs):
    sel_ref, pos_ref, place_ref, total_ref, i_ref = refs[:5]
    p_refs, refs = refs[5 : 5 + group], refs[5 + group :]
    if late:
        og_above, og_below, weight_ref = refs[:chunks], refs[chunks : 2 * chunks], refs[2 * chunks]
        refs = refs[2 * chunks + 1 :]
    go_ref, back_ref, local_ref, go_t, piece, og_buf, w_buf, late_sem, out_sem = refs
    here = pos_ref[0]
    step = pl.program_id(0)
    rows, width = total_ref.shape

    if late:
        z, groups = place_ref[0], place_ref[1]
        depth = og_buf.shape[1]
        size = rows // chunks

        def copies(arrays, source):
            cols = pl.ds(pl.multiple_of(source * depth, depth), depth)
            made = [pltpu.make_async_copy(weight_ref.at[:, cols], w_buf, late_sem.at[chunks])]
            for c in range(chunks):
                made.append(pltpu.make_async_copy(arrays[c], og_buf.at[pl.ds(c * size, size)], late_sem.at[c]))
            return made

        ends = (z == 0) | (z == groups - 1)

        @pl.when((step == 0) & (z == 0))
        def _():
            for copy in copies(og_above, groups - 1):
                copy.start()

        @pl.when((step == 0) & (z == groups - 1))
        def _():
            for copy in copies(og_below, 0):
                copy.start()

        @pl.when((step == 0) & ends)
        def _():
            for copy in copies(og_above, 0):
                copy.wait()

    def store(grad):
        low = (grad * i_ref[...]).astype(jnp.bfloat16)
        go_ref[...] = low
        for g in range(group):
            go_t[:, pl.ds(g * rows, rows)] = low[:, g * HEAD_DIM : (g + 1) * HEAD_DIM].T

    @pl.when(step * SPAN % TOPK == 0)
    def _():
        if late:
            @pl.when(ends)
            def _():
                mine = pl.ds(pl.multiple_of(step * SPAN // TOPK * width, width), width)
                store(
                    total_ref[...]
                    + lax.dot_general(og_buf[...], w_buf[mine, :], NT, preferred_element_type=jnp.float32)
                )

            @pl.when(jnp.logical_not(ends))
            def _():
                store(total_ref[...])
        else:
            store(total_ref[...])

    for part in range(SPAN):
        value_part = jnp.zeros((HEAD_DIM, BLOCK), jnp.float32)
        for g in range(group):
            value_part = value_part + jnp.dot(
                go_t[:, g * rows : (g + 1) * rows], p_refs[g][0, part, 0], preferred_element_type=jnp.float32
            )
        piece[step * SPAN + part] = value_part.T.astype(jnp.bfloat16)
    for part in range(SPAN):
        send_piece(step * SPAN + part, here, sel_ref, blocks_here, piece, back_ref, local_ref, out_sem)


def shapes_back(devices, kv_local):
    tall = kv_local * BLOCK
    return [
        jax.ShapeDtypeStruct((devices, tall, HEAD_DIM), jnp.bfloat16),
        jax.ShapeDtypeStruct((TOPK, tall, HEAD_DIM), jnp.bfloat16),
    ]


def weight_blocks(group, rows, span):
    return [
        pl.BlockSpec(
            (1, span, 1, rows, BLOCK),
            functools.partial(lambda g, s: (s * span // TOPK, s % (TOPK // span), g, 0, 0), g),
        )
        for g in range(group)
    ]


def value_grads(kv_local, devices, blocks_here, selected, position, place, total, weighed, late, weight):
    rows, q_cols = total.shape
    width = q_cols // kv_local
    group = width // HEAD_DIM
    weights, _, inverse, _, _ = weighed
    column_block = pl.BlockSpec((rows, width), lambda s: (0, s * SPAN // TOPK))
    operands = [selected, position, place, total, inverse] + [weights] * group
    in_specs = [
        SMEM, SMEM, SMEM, column_block, column_block, *weight_blocks(group, rows, SPAN),
    ]
    chunks, depth = 1, HEAD_DIM
    if late is not None:
        chunks, depth = len(late[0]), late[0][0].shape[1]
        extra = [*late[0], *late[1], weight]
        operands += extra
        in_specs += [ANY] * (len(extra) - 1) + [HBM]
    steps = kv_local * TOPK
    return pl.pallas_call(
        functools.partial(values_kernel, blocks_here, group, chunks, late is not None),
        grid=(steps // SPAN,),
        out_shape=[jax.ShapeDtypeStruct((rows, q_cols), jnp.bfloat16)] + shapes_back(devices, kv_local),
        in_specs=in_specs,
        out_specs=[column_block, HBM, HBM],
        scratch_shapes=[
            pltpu.VMEM((HEAD_DIM, group * rows), jnp.bfloat16),
            pltpu.VMEM((steps, BLOCK, HEAD_DIM), jnp.bfloat16),
            pltpu.VMEM((rows, depth), jnp.bfloat16),
            pltpu.VMEM((q_cols, depth), jnp.bfloat16),
            pltpu.SemaphoreType.DMA((chunks + 1,)),
            pltpu.SemaphoreType.DMA((steps,)),
        ],
        compiler_params=pltpu.CompilerParams(vmem_limit_bytes=VMEM_LIMIT),
        name="values",
    )(*operands)


def keys_kernel(blocks_here, group, *refs):
    sel_ref, pos_ref, q_ref, go_ref, o_ref, k_ref, v_ref = refs[:7]
    p_refs, refs = refs[7 : 7 + group], refs[7 + group :]
    dq_ref, back_ref, local_ref, q_t, dot_buf, ds_buf, dq_acc, piece, out_sem = refs
    here = pos_ref[0]
    step = pl.program_id(0)
    rows, _ = q_ref.shape
    factor = HEAD_DIM ** (-0.5)

    @pl.when(step % TOPK == 0)
    def _():
        for g in range(group):
            at = slice(g * HEAD_DIM, (g + 1) * HEAD_DIM)
            q_t[:, pl.ds(g * rows, rows)] = q_ref[:, at].T
            row_dot = jnp.sum(go_ref[:, at].astype(jnp.float32) * o_ref[:, at], axis=1, keepdims=True)
            dot_buf[g] = jnp.broadcast_to(row_dot, (rows, HEAD_DIM))
        dq_acc[...] = jnp.zeros_like(dq_acc)

    keys_here = k_ref[0]
    values_here = v_ref[0]

    def grad_weights(g):
        return lax.dot_general(
            go_ref[:, g * HEAD_DIM : (g + 1) * HEAD_DIM], values_here, NT, preferred_element_type=jnp.float32
        )

    later = grad_weights(0)
    for g in range(group):
        at = slice(g * HEAD_DIM, (g + 1) * HEAD_DIM)
        now = later
        if g + 1 < group:
            later = grad_weights(g + 1)
        row_dot = jnp.concatenate([dot_buf[g]] * (BLOCK // HEAD_DIM), axis=1)
        grad_low = (p_refs[g][0, 0, 0].astype(jnp.float32) * (now - row_dot)).astype(jnp.bfloat16)
        ds_buf[pl.ds(g * rows, rows)] = grad_low
        dq_acc[:, at] += jnp.dot(grad_low, keys_here, preferred_element_type=jnp.float32)
    key_part = jnp.dot(q_t[...], ds_buf[...], preferred_element_type=jnp.float32)
    piece[step] = (key_part.T * factor).astype(jnp.bfloat16)

    @pl.when(step % TOPK == TOPK - 1)
    def _():
        dq_ref[...] = (dq_acc[...] * factor).astype(jnp.bfloat16)

    send_piece(step, here, sel_ref, blocks_here, piece, back_ref, local_ref, out_sem)


def key_grads(kv_local, devices, blocks_here, selected, position, queries, grad_output, weighed):
    rows, q_cols = queries.shape
    width = q_cols // kv_local
    group = width // HEAD_DIM
    weights, attended, _, key_slots, value_slots = weighed
    column_block = pl.BlockSpec((rows, width), lambda s: (0, s // TOPK))
    slot_block = pl.BlockSpec((1, BLOCK, HEAD_DIM), lambda s: (s // TOPK, s % TOPK, 0))
    steps = kv_local * TOPK
    return pl.pallas_call(
        functools.partial(keys_kernel, blocks_here, group),
        grid=(steps,),
        out_shape=[jax.ShapeDtypeStruct((rows, q_cols), jnp.bfloat16)] + shapes_back(devices, kv_local),
        in_specs=[
            SMEM, SMEM, column_block, column_block, column_block, slot_block, slot_block,
            *weight_blocks(group, rows, 1),
        ],
        out_specs=[column_block, HBM, HBM],
        scratch_shapes=[
            pltpu.VMEM((HEAD_DIM, group * rows), jnp.bfloat16),
            pltpu.VMEM((group, rows, HEAD_DIM), jnp.float32),
            pltpu.VMEM((group * rows, BLOCK), jnp.bfloat16),
            pltpu.VMEM((rows, width), jnp.float32),
            pltpu.VMEM((steps, BLOCK, HEAD_DIM), jnp.bfloat16),
            pltpu.SemaphoreType.DMA((steps,)),
        ],
        compiler_params=pltpu.CompilerParams(vmem_limit_bytes=VMEM_LIMIT),
        name="keys",
    )(selected, position, queries, grad_output, attended, key_slots, value_slots, *[weights] * group)


def collect_kernel(kv_local, devices, blocks_here, sel_ref, pos_ref, local_ref, recv_ref, out_ref, pieces, acc, low, in_sem, out_sem):
    here = pos_ref[0]
    total = TOPK + devices - 1

    def source(index):
        if index < TOPK:
            block = sel_ref[here, index]
            return block % blocks_here, block // blocks_here == here
        row = here + (index - TOPK + 1)
        inner = pick_of(sel_ref, jnp.minimum(row, devices - 1), here, blocks_here)
        return inner, (row < devices) & (inner >= 0)

    def fetch(index):
        src = local_ref.at[index] if index < TOPK else recv_ref.at[here + (index - TOPK + 1)]
        return pltpu.make_async_copy(src, pieces.at[index], in_sem.at[index])

    for index in range(total):
        @pl.when(source(index)[1])
        def _():
            fetch(index).start()

    acc[...] = jnp.zeros_like(acc)
    for index in range(total):
        inner, there = source(index)

        @pl.when(there)
        def _():
            fetch(index).wait()
            acc[inner] += pieces[index].astype(jnp.float32)

    def store(block):
        rows = pl.ds(block * BLOCK, BLOCK)
        return [
            pltpu.make_async_copy(
                low.at[block, pl.ds(head * BLOCK, BLOCK)],
                out_ref.at[rows, pl.ds(head * HEAD_DIM, HEAD_DIM)],
                out_sem.at[block, head],
            )
            for head in range(kv_local)
        ]

    for block in range(blocks_here):
        low[block] = acc[block].astype(jnp.bfloat16)
        for copy in store(block):
            copy.start()
    for block in range(blocks_here):
        for copy in store(block):
            copy.wait()


def collect(kv_local, devices, blocks_here, selected, position, local, recv):
    tall = kv_local * BLOCK
    return pl.pallas_call(
        functools.partial(collect_kernel, kv_local, devices, blocks_here),
        out_shape=jax.ShapeDtypeStruct((blocks_here * BLOCK, kv_local * HEAD_DIM), jnp.bfloat16),
        in_specs=[SMEM, SMEM, HBM, ANY],
        out_specs=HBM,
        scratch_shapes=[
            pltpu.VMEM((TOPK + devices - 1, tall, HEAD_DIM), jnp.bfloat16),
            pltpu.VMEM((blocks_here, tall, HEAD_DIM), jnp.float32),
            pltpu.VMEM((blocks_here, tall, HEAD_DIM), jnp.bfloat16),
            pltpu.SemaphoreType.DMA((TOPK + devices - 1,)),
            pltpu.SemaphoreType.DMA((blocks_here, kv_local)),
        ],
        compiler_params=pltpu.CompilerParams(vmem_limit_bytes=VMEM_LIMIT),
    )(selected, position, local, recv)


def body(queries, keys, values, out_grad, out_weight, selected):
    kv_cols = keys.shape[1]
    kv_local = kv_cols // HEAD_DIM
    blocks_here = keys.shape[0] // BLOCK
    devices = lax.axis_size("seq")
    groups = lax.axis_size("head")
    position = lax.axis_index("seq").astype(jnp.int32).reshape(1)
    place = jnp.stack([lax.axis_index("head"), jnp.int32(groups)]).astype(jnp.int32)

    rows = out_grad.shape[0] // CHUNKS
    own = [out_grad[c * rows : (c + 1) * rows] for c in range(CHUNKS)]
    above, below = {0: own}, {0: own}
    for step in range(1, groups):
        up = [(z, z + 1) for z in range(step - 1, groups - 1)]
        down = [(z, z - 1) for z in range(1, groups - step + 1)]
        below[step], above[step] = [], []
        for c in range(CHUNKS):
            below[step].append(lax.ppermute(below[step - 1][c], "head", up))
            above[step].append(lax.ppermute(above[step - 1][c], "head", down))

    def trade(array):
        return lax.all_to_all(array, "seq", split_axis=0, concat_axis=0, tiled=True)

    recv = [trade(pack(head, devices, blocks_here, selected, position, keys, values)) for head in range(kv_local)]

    early = [0] + [t for s in range(1, groups - 1) for t in (-s, s)]
    arrays = [below[-t] if t < 0 else above[t] for t in early]
    total = project(tuple(early), arrays, out_weight, place)
    late = (above[groups - 1], below[groups - 1]) if groups > 1 else None
    weighed = None
    for head in range(kv_local):
        weighed = weigh(head, kv_local, blocks_here, selected, position, queries, keys, values, recv[head], weighed)

    grad_output, back_values, local_values = value_grads(
        kv_local, devices, blocks_here, selected, position, place, total, weighed, late, out_weight
    )
    arrived_values = trade(back_values)
    query_grad, back_keys, local_keys = key_grads(
        kv_local, devices, blocks_here, selected, position, queries, grad_output, weighed
    )
    arrived_keys = trade(back_keys)
    value_grad = collect(kv_local, devices, blocks_here, selected, position, local_values, arrived_values)
    key_grad = collect(kv_local, devices, blocks_here, selected, position, local_keys, arrived_keys)
    return (query_grad, key_grad, value_grad)


def solution(mesh):
    in_specs = (
        P("seq", "head"),
        P("seq", "head"),
        P("seq", "head"),
        P("seq", "head"),
        P("head", None),
        P(),
    )
    out_specs = (P("seq", "head"), P("seq", "head"), P("seq", "head"))
    return jax.shard_map(body, mesh=mesh, in_specs=in_specs, out_specs=out_specs, check_vma=False)
```
